32 devices in a mesh: dp: 16 (over z, y, x), rep: 2 (over core).
Axes of the slice: x: 2, y: 2, z: 4, core: 2. Of those that a mesh axis runs over, the one named last changes fastest.
Arguments:
- row_grads: float32 [16384, 512], P(('dp', 'rep')), may hold values from -2500 to 2500
- token_owner: int32 [16384, 1], P(('dp', 'rep')), may hold values from 0 to 15; in each aligned block of 512 rows (0 to 511, 512 to 1023, ...) at most 64 rows name the same one
- token_row: int32 [16384], P(('dp', 'rep')), may hold values from 0 to 8191
- table: float32 [131072, 512], P('dp'), may hold values from -6 to 6
- moment: float32 [131072, 512], P('dp'), may hold values from -3 to 3
- second: float32 [131072, 512], P('dp'), may hold values from 0.05 to 2
Outputs:
- new_table: float32 [131072, 512], P('dp')
- new_moment: float32 [131072, 512], P('dp')
- new_second: float32 [131072, 512], P('dp')
The draws below stay inside these ranges and needn't reach their ends.
Inputs may be any that keep to these rules, and one draw needn't show every extreme that they name: `token_owner`: among the rows of one device at most 64 name one owner; in every draw some owner is named by exactly 64 rows of some device.
All inputs are finite; a program needn't handle non-finite values.
Results may differ from the reference program's by a relative error of at most 0.00007.
Values sent between devices are 32-bit elements; how exact they have to be, the bound alone decides.
A program may use at most 192 MiB of HBM per device.

```python
import math
import jax
import jax.numpy as jnp
import numpy as np

VOCAB = 131072
ADAM_STEP = 100
TOK_DEV = 512
LW = 512
TOKENS = 16384
ROWS_OWN = 8192
CAP = 64
N_DP = 16
N_REP = 2


def draw_row_grads(key, part):
    keys = jax.random.split(key, 5)
    row_scale = jnp.exp(jax.random.uniform(keys[0], (TOKENS, 1), jnp.float32, 0.0, math.log(10.0)))
    col_scale = jnp.exp(jax.random.uniform(keys[1], (1, LW), jnp.float32, 0.0, math.log(10.0)))
    device_pos = (jnp.arange(TOKENS) // TOK_DEV).astype(jnp.float32)
    ramp = (1.0 + 2.0 * device_pos / max(N_DP * N_REP - 1, 1))[:, None]
    base = jnp.clip(jax.random.normal(keys[4], (TOKENS, LW), jnp.float32), -4.0, 4.0)
    return (base * row_scale * col_scale * ramp).astype(jnp.float32)


def place_ends(drawn, key, least, top_value):
    shape = drawn.shape
    spot = [jax.random.randint(jax.random.fold_in(key, axis), (), 0, shape[axis]) for axis in range(len(shape))]
    drawn = drawn.at[tuple(spot)].set(least)
    longest = shape.index(max(shape))
    spot[longest] = (spot[longest] + 1) % shape[longest]
    return drawn.at[tuple(spot)].set(top_value)


def steps_of(stream_key, shape, shards, least, top_value):
    loudness, own = 1.0, jax.random.fold_in(stream_key, 6)
    for axis_at, blocks in shards:
        heights = jnp.exp(jax.random.uniform(jax.random.fold_in(own, axis_at), (blocks,), jnp.float32, least / len(shards), top_value / len(shards)))
        loudness = loudness * jnp.repeat(heights, shape[axis_at] // blocks).reshape([-1 if axis == axis_at else 1 for axis in range(len(shape))])
    return loudness


def cumulative_ranks(number_of, slope):
    portions = [(1 << 20) // math.isqrt(grade ** slope) + 1 for grade in range(1, number_of + 1)]
    spread = 1 + sum(portions) // (1 << 30)
    return np.cumsum(np.array([max(1, weight // spread) for weight in portions]))


def skewed_ids(rng, shape, amount, lean):
    grid = cumulative_ranks(amount, lean)
    lot = jax.random.randint(jax.random.fold_in(rng, 1), shape, 0, int(grid[amount - 1]))
    grade = jnp.searchsorted(jnp.asarray(grid, jnp.int32), lot, side="right")
    return jax.random.permutation(jax.random.fold_in(rng, 2), amount)[grade].astype(jnp.int32)


def deal_out(stream_key, own, number, rows, count, top, most, lean):
    order = jax.random.permutation(stream_key, count)
    packed, usual = load_shares(count, rows * top, most, lean, True), load_shares(count, rows * top, most, lean, False)
    places = jnp.arange(count)

    def named(lengths, rotation):
        used = int((lengths > 0).sum())
        fixed = max(1, used // 4)
        moved = fixed + (places - fixed + rotation * (used - fixed)) % max(1, count - fixed)
        return jnp.zeros((count,), jnp.int32).at[order[jnp.where(places < fixed, places, moved)]].set(jnp.asarray(lengths, jnp.int32))

    lengths = jnp.where(number % 4 == 0, named(packed, number // 4), named(usual, number - number // 4 - 1))
    mixed = jax.random.permutation(jax.random.fold_in(own, 3), count)
    source_of, sink = mixed[0:count // 2 * 2:2], mixed[1:count // 2 * 2:2]
    slack = jnp.minimum(lengths[source_of] - 1, most - lengths[sink]) // 2
    slack = jnp.where((source_of == order[0]) | (sink == order[0]) | (lengths[sink] == 0), 0, jnp.maximum(slack, 0))
    moved = jax.random.randint(jax.random.fold_in(own, 4), (count // 2,), 0, 1 << 20) % (slack + 1)
    lengths = lengths.at[source_of].add(-moved).at[sink].add(moved)
    labels = jnp.searchsorted(jnp.cumsum(lengths), jnp.arange(rows * top), side="right").astype(jnp.int32)
    grid = labels.reshape(top, rows).T
    grid = grid[jax.random.permutation(jax.random.fold_in(own, 1), rows)]
    rotation = jax.random.randint(jax.random.fold_in(own, 2), (rows, 1), 0, top)
    return jnp.take_along_axis(grid, (jnp.arange(top)[None, :] + rotation) % top, axis=1)


def load_shares(amount, total, most, slope, full):
    weights = [(1 << 20) // math.isqrt(rank ** slope) + 1 for rank in range(1, amount + 1)]
    largest = most if full else min(most, max(-(-total // amount), total * weights[0] // sum(weights)))
    least = 1 if total - largest >= amount - 1 else 0
    holding, spare = [largest] + [least] * (amount - 1), total - largest - least * (amount - 1)
    while spare > 0:
        movable = [i for i in range(1, amount) if holding[i] < largest] or [i for i in range(1, amount) if holding[i] < most]
        pool, budget = sum([weights[i] for i in movable]), spare
        for i in movable:
            extra = min(most - holding[i], max(1, budget * weights[i] // pool), spare)
            holding[i] = holding[i] + extra
            spare = spare - extra
    return np.array(holding)


def noise(rng, dims, deviation, bound, pieces=(), kind=jnp.bfloat16):
    drawn = deviation * jax.random.normal(rng, dims, jnp.float32)
    if pieces:
        drawn = drawn * steps_of(rng, dims, pieces, -0.22, 0.18)
    return jnp.clip(drawn, -bound, bound).astype(kind)


def setup_inputs(seed: int = 0) -> dict:
    splits = jax.random.split(jax.random.key(seed), 7)
    row_grads = draw_row_grads(jax.random.fold_in(splits[6], 71), 0)
    token_owner_keys = jax.random.split(jax.random.fold_in(splits[1], 1), TOKENS // TOK_DEV)
    token_owner_turns = jax.random.permutation(jax.random.fold_in(splits[1], 3), TOKENS // TOK_DEV)
    token_owner = jax.vmap(lambda own, number: deal_out(jax.random.fold_in(splits[1], 2), own, number, TOK_DEV, N_DP, 1, CAP, 2))(token_owner_keys, token_owner_turns).reshape((TOKENS, 1))
    token_row = place_ends(skewed_ids(splits[2], (TOKENS,), ROWS_OWN, 2), jax.random.fold_in(splits[2], 3), 0, ROWS_OWN - 1).astype(jnp.int32)
    table = noise(splits[3], (VOCAB, LW), 1.0, 6.0, ((0, 16),), jnp.float32)
    moment = noise(splits[4], (VOCAB, LW), 0.5, 3.0, ((0, 16),), jnp.float32)
    second = jnp.clip(jnp.exp(math.log(2.0) - 3.6888794 * jax.random.uniform(splits[5], (VOCAB, LW), jnp.float32) ** steps_of(splits[5], (VOCAB, LW), ((0, 16),), -0.2, 0.2)), 0.05, 2.0)
    return {"row_grads": row_grads, "token_owner": token_owner, "token_row": token_row, "table": table, "moment": moment, "second": second}


def reference(row_grads, token_owner, token_row, table, moment, second):
    row_id = (token_owner[:, 0] * ROWS_OWN + token_row).astype(jnp.int32)
    dense = jnp.zeros((VOCAB, LW), jnp.float32).at[row_id].add(row_grads.astype(jnp.float32))
    norm = jnp.sqrt(jnp.sum(dense * dense))
    limit = 0.5 * jnp.sqrt(jnp.float32(VOCAB * LW))
    clip = jnp.minimum(jnp.float32(1.0), limit / (norm + 1e-06))
    clipped = clip * dense
    new_moment = 0.9 * moment + 0.1 * clipped
    new_second = 0.999 * second + 0.001 * clipped * clipped
    first_fix = 1.0 - 0.9 ** ADAM_STEP
    second_fix = 1.0 - 0.999 ** ADAM_STEP
    update = new_moment / first_fix / (jnp.sqrt(new_second / second_fix) + 1e-08)
    new_table = table - 0.01 * (update + 0.01 * table)
    return (new_table, new_moment, new_second)
```

```python
import functools

import jax
import jax.numpy as jnp
from jax import lax
from jax.experimental import pallas as pl
from jax.experimental.pallas import tpu as pltpu
from jax.sharding import PartitionSpec as P

ADAM_STEP = 100
SMEM = pl.BlockSpec(memory_space=pltpu.SMEM)
VMEM = pl.BlockSpec(memory_space=pltpu.VMEM)
ANY = pl.BlockSpec(memory_space=pl.ANY)
MIB = 1 << 20


def pack_kernel(owners, capacity, owner_ref, row_ref, grads_ref, rows_out, ids_out):
    def clear(o, carry):
        ids_out[o, capacity] = 0
        return carry

    lax.fori_loop(0, owners, clear, 0)

    def token(t, carry):
        o = owner_ref[t]
        p = ids_out[o, capacity]
        ids_out[o, capacity] = p + 1
        ids_out[o, p] = row_ref[t]
        rows_out[pl.ds(o * capacity + p, 1), :] = grads_ref[pl.ds(t, 1), :]
        return carry

    lax.fori_loop(0, owner_ref.shape[0], token, 0, unroll=4)


def pack(row_grads, owner_ids, token_row, owners, capacity):
    tokens, cols = row_grads.shape
    return pl.pallas_call(
        functools.partial(pack_kernel, owners, capacity),
        out_shape=(
            jax.ShapeDtypeStruct((owners * capacity, cols), jnp.float32),
            jax.ShapeDtypeStruct((owners, capacity + 1), jnp.int32),
        ),
        in_specs=[SMEM, SMEM, VMEM],
        out_specs=(VMEM, SMEM),
        compiler_params=pltpu.CompilerParams(vmem_limit_bytes=6 * MIB),
    )(owner_ids, token_row, row_grads)


def sum_kernel(owners, capacity, rep_ref, own_ids, other_ids, own_ref, other_ref, out_ref, total_ref, dense_ref, sem):
    rows, cols = out_ref.shape
    step = 64

    def clear(i, carry):
        dense_ref[pl.ds(pl.multiple_of(i * step, step), step), :] = jnp.zeros((step, cols), jnp.float32)
        return carry

    lax.fori_loop(0, rows // step, clear, 0)

    def add(ids, ref):
        def source(s, carry):
            count = ids[s, capacity]

            def pair(j, inner):
                i = 2 * j
                r0 = ids[s, i]
                r1 = jnp.where(i + 1 < count, ids[s, i + 1], rows)
                d0 = dense_ref[pl.ds(r0, 1), :]
                d1 = dense_ref[pl.ds(r1, 1), :]
                n0 = d0 + ref[pl.ds(s * capacity + i, 1), :]
                n1 = jnp.where(r0 == r1, n0, d1) + ref[pl.ds(s * capacity + i + 1, 1), :]
                dense_ref[pl.ds(r0, 1), :] = n0
                dense_ref[pl.ds(r1, 1), :] = n1
                return inner

            return lax.fori_loop(0, (count + 1) // 2, pair, carry)

        lax.fori_loop(0, owners, source, 0)

    for core in range(2):
        mine = rep_ref[0] == core

        @pl.when(mine)
        def _():
            add(own_ids, own_ref)

        @pl.when(jnp.logical_not(mine))
        def _():
            add(other_ids, other_ref)

    copy = pltpu.make_async_copy(dense_ref.at[pl.ds(0, rows)], out_ref, sem)
    copy.start()

    def square(i, acc):
        block = dense_ref[pl.ds(pl.multiple_of(i * step, step), step), :]
        return acc + jnp.sum((block * block).reshape(step // 8, 8, cols), axis=0)

    acc = lax.fori_loop(0, rows // step, square, jnp.zeros((8, cols), jnp.float32))
    total_ref[0, 0] = jnp.sum(acc)
    copy.wait()


def accumulate(rep, own_ids, other_ids, own, other, rows):
    owners, width = own_ids.shape
    cols = own.shape[1]
    return pl.pallas_call(
        functools.partial(sum_kernel, owners, width - 1),
        out_shape=(
            jax.ShapeDtypeStruct((rows, cols), jnp.float32),
            jax.ShapeDtypeStruct((1, 1), jnp.float32),
        ),
        in_specs=[SMEM, SMEM, SMEM, VMEM, VMEM],
        out_specs=(ANY, SMEM),
        scratch_shapes=[pltpu.VMEM((rows + 8, cols), jnp.float32), pltpu.SemaphoreType.DMA],
        compiler_params=pltpu.CompilerParams(vmem_limit_bytes=58 * MIB),
    )(rep, own_ids, other_ids, own, other)


def adamw(clip, dense, moment, second, table):
    g = clip * dense
    new_moment = 0.9 * moment + 0.1 * g
    new_second = 0.999 * second + 0.001 * g * g
    first_fix = 1.0 - 0.9**ADAM_STEP
    second_fix = 1.0 - 0.999**ADAM_STEP
    update = new_moment / first_fix / (jnp.sqrt(new_second / second_fix) + 1e-08)
    return (table - 0.01 * (update + 0.01 * table), new_moment, new_second)


def local(row_grads, token_owner, token_row, table, moment, second):
    owners = lax.axis_size("dp")
    tokens, cols = row_grads.shape
    capacity = 2 * tokens // owners
    send_rows, send_ids = pack(row_grads, token_owner.reshape(tokens), token_row, owners, capacity)
    got = lax.all_to_all(
        send_rows.reshape(owners, capacity, cols), "dp", split_axis=0, concat_axis=0, tiled=True
    ).reshape(owners * capacity, cols)
    got_ids = lax.all_to_all(send_ids, "dp", split_axis=0, concat_axis=0, tiled=True)
    swap = [(0, 1), (1, 0)]
    other_ids = lax.ppermute(got_ids, "rep", swap)
    other = lax.ppermute(got, "rep", swap)
    rep = lax.axis_index("rep").reshape(1).astype(jnp.int32)
    dense, total = accumulate(rep, got_ids, other_ids, got, other, table.shape[0])
    totals = lax.all_to_all(
        jnp.broadcast_to(total.reshape(1, 1, 1), (owners, 1, 128)), "dp", split_axis=0, concat_axis=0, tiled=True
    )
    total = jnp.sum(totals[:, 0, :1], axis=0, keepdims=True)
    entries = owners * table.shape[0] * cols
    limit = 0.5 * jnp.sqrt(jnp.float32(entries))
    clip = jnp.minimum(jnp.float32(1.0), limit / (jnp.sqrt(total) + 1e-06))
    return adamw(clip, dense, moment, second, table)


def solution(mesh):
    return jax.shard_map(
        local,
        mesh=mesh,
        in_specs=(
            P(("dp", "rep"), None),
            P(("dp", "rep"), None),
            P(("dp", "rep")),
            P("dp", None),
            P("dp", None),
            P("dp", None),
        ),
        out_specs=(P("dp", None), P("dp", None), P("dp", None)),
        check_vma=False,
    )
```
